16 devices in a mesh: dp: 4 (over y, z, core), tp: 4 (over x).
Axes of the slice: x: 4, y: 2, z: 1, core: 2. Of those that a mesh axis runs over, the one named last changes fastest.
The devices are a block of a 4x4x8 slice.
Arguments:
- x: bfloat16 [4096, 4096], P(('dp', 'tp')), parts along dimension 0
- dy: bfloat16 [4096, 4096], P(('dp', 'tp')), parts along dimension 0
- gate: bfloat16 [4096, 12800], P('dp', 'tp'), parts along dimension 0
- up: bfloat16 [4096, 12800], P('dp', 'tp'), parts along dimension 0
- w_gate: bfloat16 [4096, 12800], P(None, 'tp')
- w_up: bfloat16 [4096, 12800], P(None, 'tp')
- w_down: bfloat16 [12800, 4096], P('tp')
Outputs:
- output 1: bfloat16 [4096, 4096], P(('dp', 'tp')), parts along dimension 0
- output 2: bfloat16 [16384, 12800], P('dp', 'tp'), parts along dimension 0
- output 3: bfloat16 [16384, 12800], P('dp', 'tp'), parts along dimension 0
- output 4: bfloat16 [51200, 4096], P(('dp', 'tp')), parts along dimension 0
There are 4 independent parts. The reference program is written for one: setup_inputs(seed, part) draws one part's arguments, and reference() takes and returns one part's arrays. A program takes and returns all parts, laid end to end along the dimension named above; an argument that names none is the same for every part.
All inputs are finite; a program needn't handle non-finite values.
Results may differ from the reference program's by a relative error of at most 0.012.
Values are sent between devices in bfloat16 or wider.
A program may use at most 768 MiB of HBM per device.

```python
import jax
import jax.numpy as jnp

ROWS = 1024
D = 4096
FF = 12800


def act(gate, up):
    return jax.nn.silu(gate) * up


def setup_inputs(seed: int = 0, part: int = 0) -> dict:
    kx, ky, ka, kb, kg, ku, kd = jax.random.split(jax.random.key(seed), 7)
    kx, ky, ka, kb = (jax.random.fold_in(k, part) for k in (kx, ky, ka, kb))
    drawn = {
        "x": jax.random.normal(kx, (ROWS, D), jnp.float32),
        "dy": jax.random.normal(ky, (ROWS, D), jnp.float32),
        "gate": jax.random.normal(ka, (ROWS, FF), jnp.float32),
        "up": jax.random.normal(kb, (ROWS, FF), jnp.float32),
        "w_gate": jax.random.normal(kg, (D, FF), jnp.float32) * D**-0.5,
        "w_up": jax.random.normal(ku, (D, FF), jnp.float32) * D**-0.5,
        "w_down": jax.random.normal(kd, (FF, D), jnp.float32) * FF**-0.5,
    }
    return {k: v.astype(jnp.bfloat16) for k, v in drawn.items()}


def reference(x, dy, gate, up, w_gate, w_up, w_down):
    hidden, back = jax.vjp(act, gate.astype(jnp.float32), up.astype(jnp.float32))
    d_hidden = jnp.dot(dy, w_down.T, preferred_element_type=jnp.float32)
    d_gate, d_up = (g.astype(jnp.bfloat16) for g in back(d_hidden))
    dx = jnp.dot(d_gate, w_gate.T, preferred_element_type=jnp.float32) + jnp.dot(d_up, w_up.T, preferred_element_type=jnp.float32)
    dw_gate = jnp.dot(x.T, d_gate, preferred_element_type=jnp.float32)
    dw_up = jnp.dot(x.T, d_up, preferred_element_type=jnp.float32)
    dw_down = jnp.dot(hidden.astype(jnp.bfloat16).T, dy, preferred_element_type=jnp.float32)
    return tuple(g.astype(jnp.bfloat16) for g in (dx, dw_gate, dw_up, dw_down))
```

```python
import functools

import jax
import jax.numpy as jnp
from jax import lax
from jax.experimental import pallas as pl
from jax.experimental.pallas import tpu as pltpu
from jax.sharding import PartitionSpec as P

BF16, F32 = jnp.bfloat16, jnp.float32
VMEM_LIMIT = 67_000_000


def nt(a, b):
    return lax.dot_general(a, b, (((1,), (1,)), ((), ())), preferred_element_type=F32)


def tn(a, b):
    return lax.dot_general(a, b, (((0,), (0,)), ((), ())), preferred_element_type=F32)


def splits(total, step):
    starts = list(range(0, total, step))
    if len(starts) > 1 and total - starts[-1] < step // 2:
        starts.pop()
    return [(s, e - s) for s, e in zip(starts, starts[1:] + [total])]


def gather_kernel(n, a_tiles, tb, tm, tn_cols, dy0, x0, gate, up, w_down, w_gate, w_up,
                  xg, dg, du, own, mid, raw_l, raw_r, far_0, far_1, dwd,
                  dyg, hid, dgc, duc, gb, ub, xst, wa, wb, st_f, st_b,
                  s_dy, r_dy, s_x, r_x, m_in, m_gu, m_wa, m_wb, m_st, m_d, m_o):
    rows, d = dy0.shape
    ff = gate.shape[1]
    half = rows // 2
    me = lax.axis_index("tp")
    right, left = lax.rem(me + 1, n), lax.rem(me + n - 1, n)
    n_a, n_b = len(a_tiles), d // tb
    chunks = 4

    def place(c, p):
        return pl.ds(pl.multiple_of(c * rows + p * half, half), half)

    def send(src, dst, s_sem, r_sem, c, p, to):
        return pltpu.make_async_remote_copy(src_ref=src, dst_ref=dst.at[place(c, p)], send_sem=s_sem.at[c, p],
                                            recv_sem=r_sem.at[c, p], device_id={"tp": to},
                                            device_id_type=pl.DeviceIdType.MESH)

    def block_sends(src, dst, s_sem, r_sem):
        h0, h1 = src.at[pl.ds(0, half)], src.at[pl.ds(half, half)]
        return [send(h0, dst, s_sem, r_sem, 1, 0, right), send(h1, dst, s_sem, r_sem, 1, 1, left),
                send(h1, dst, s_sem, r_sem, 2, 0, right), send(h0, dst, s_sem, r_sem, 2, 1, left)]

    def forwards(buf, s_sem, r_sem):
        return [send(buf.at[place(1, 0)], buf, s_sem, r_sem, 3, 0, right),
                send(buf.at[place(1, 1)], buf, s_sem, r_sem, 3, 1, left)]

    def arrived(buf, r_sem, c):
        for p in range(2):
            pltpu.make_async_copy(buf.at[place(c, p)], buf.at[place(c, p)], r_sem.at[c, p]).wait()

    def load_a(t, slot):
        start, size = a_tiles[t]
        return pltpu.make_async_copy(w_down.at[pl.ds(start, size)], wa.at[slot, pl.ds(0, size)], m_wa.at[slot])

    def load_b(j, slot):
        at = pl.ds(pl.multiple_of(j * tb, tb), tb)
        return [pltpu.make_async_copy(w.at[at], wb.at[slot, k], m_wb.at[slot, k]) for k, w in enumerate((w_gate, w_up))]

    def load_gu(c):
        later, last = (c + 2) // 3, c // 3
        flip = (c // 2) * (1 - last)
        copies = []
        for p, (shift, h) in enumerate(((later * (n - 1) - last * (n - 3), flip), (later + last, 1 - flip))):
            at = pl.ds(pl.multiple_of(lax.rem(me + shift, n) * rows + h * half, half), half)
            for k, (src, dst) in enumerate(((gate, gb), (up, ub))):
                copies.append(pltpu.make_async_copy(src.at[at], dst.at[pl.ds(p * half, half)], m_gu.at[p, k]))
        return copies

    def save_d(c):
        at = pl.ds(pl.multiple_of(c * rows, rows), rows)
        return [pltpu.make_async_copy(dgc, dg.at[at], m_d.at[0]), pltpu.make_async_copy(duc, du.at[at], m_d.at[1])]

    def save_f(dst, j, slot):
        at = pl.ds(pl.multiple_of(j * tb, tb), tb)
        return pltpu.make_async_copy(st_f.at[slot], dst.at[:, at], m_st.at[slot, 0])

    def save_b(dst0, dst1, j, slot):
        at = pl.ds(pl.multiple_of(j * tb, tb), tb)
        return [pltpu.make_async_copy(st_b.at[slot, pl.ds(p * half, half)], dst.at[:, at], m_st.at[slot, p])
                for p, dst in enumerate((dst0, dst1))]

    first_dy = pltpu.make_async_copy(dy0, dyg.at[pl.ds(0, rows)], m_in.at[0])
    first_x = pltpu.make_async_copy(x0, xst, m_in.at[1])
    keep_x = pltpu.make_async_copy(xst, xg.at[pl.ds(0, rows)], m_in.at[2])
    first_dy.start()
    load_a(0, 0).start()
    for c in load_gu(0):
        c.start()
    first_x.start()
    load_a(1, 1).start()
    for c in load_b(0, 0) + load_b(1, 1):
        c.start()

    barrier = pltpu.get_barrier_semaphore()
    for other in (left, right):
        pl.semaphore_signal(barrier, inc=1, device_id={"tp": other}, device_id_type=pl.DeviceIdType.MESH)
    pl.semaphore_wait(barrier, 2)
    for c in block_sends(dy0, dyg, s_dy, r_dy):
        c.start()
    first_x.wait()
    keep_x.start()
    first_dy.wait()

    def chunk(c, carry):
        @pl.when(c > 0)
        def _():
            arrived(dyg, r_dy, c)

        @pl.when(c == 1)
        def _():
            for k in forwards(dyg, s_dy, r_dy):
                k.start()
            for k in block_sends(xst, xg, s_x, r_x):
                k.start()

        for k in load_gu(c):
            k.wait()
        dy = dyg.at[pl.ds(pl.multiple_of(c * rows, rows), rows)]

        for t, (start, size) in enumerate(a_tiles):
            slot = lax.rem(c * n_a + t, 2)
            load_a(t, slot).wait()
            for s, w in splits(size, 512):
                cols = pl.ds(start + s, w)
                d_hidden = nt(dy[...], wa[slot, pl.ds(s, w)])
                g, u = gb[:, cols].astype(F32), ub[:, cols].astype(F32)
                sig = jax.nn.sigmoid(g)
                silu = g * sig
                hid[pl.ds(pl.multiple_of(c * rows, rows), rows), cols] = (silu * u).astype(BF16)
                duc[:, cols] = (d_hidden * silu).astype(BF16)
                dgc[:, cols] = (d_hidden * u * (sig + silu * (1.0 - sig))).astype(BF16)
            t2 = t + 2
            if t2 < n_a:
                load_a(t2, slot).start()
            else:
                @pl.when(c < chunks - 1)
                def _():
                    load_a(t2 - n_a, slot).start()

        for k in save_d(c):
            k.start()

        @pl.when(c < chunks - 1)
        def _():
            for k in load_gu(c + 1):
                k.start()

        def part(j, carry):
            slot = lax.rem(j, 2)
            for k in load_b(j, slot):
                k.wait()

            @pl.when(j >= 2)
            def _():
                @pl.when(lax.rem(c, 2) == 0)
                def _():
                    save_f(own, j, slot).wait()

                @pl.when(lax.rem(c, 2) == 1)
                def _():
                    for k in save_b(raw_l, raw_r, j, slot):
                        k.wait()

            r = nt(dgc[...], wb[slot, 0]) + nt(duc[...], wb[slot, 1])

            @pl.when(lax.rem(c, 2) == 0)
            def _():
                st_f[slot] = r

            @pl.when(lax.rem(c, 2) == 1)
            def _():
                st_b[slot] = r.astype(BF16)

            @pl.when(c == 0)
            def _():
                save_f(own, j, slot).start()

            @pl.when(c == 2)
            def _():
                save_f(mid, j, slot).start()

            @pl.when(c == 1)
            def _():
                for k in save_b(raw_l, raw_r, j, slot):
                    k.start()

            @pl.when(c == 3)
            def _():
                for k in save_b(far_0, far_1, j, slot):
                    k.start()

            @pl.when(c * n_b + j + 2 < chunks * n_b)
            def _():
                for k in load_b(lax.rem(j + 2, n_b), slot):
                    k.start()
            return carry

        lax.fori_loop(0, n_b, part, 0)
        for slot in range(2):
            @pl.when(lax.rem(c, 2) == 0)
            def _():
                save_f(own, 0, slot).wait()

            @pl.when(lax.rem(c, 2) == 1)
            def _():
                for k in save_b(raw_l, raw_r, 0, slot):
                    k.wait()
        for k in save_d(c):
            k.wait()
        return carry

    lax.fori_loop(0, chunks, chunk, 0)

    arrived(xg, r_x, 1)
    for k in forwards(xg, s_x, r_x):
        k.start()

    def save_w(i, slot):
        at = pl.ds(pl.multiple_of(i * tm, tm), tm)
        return pltpu.make_async_copy(wa.at[slot, pl.ds(0, tm)], dwd.at[at], m_o.at[slot])

    def down(i, carry):
        slot = lax.rem(i, 2)

        @pl.when(i >= 2)
        def _():
            save_w(i, slot).wait()

        def cols(k, carry):
            at = pl.ds(pl.multiple_of(k * tn_cols, tn_cols), tn_cols)
            mine = pl.ds(pl.multiple_of(i * tm, tm), tm)
            wa[slot, pl.ds(0, tm), at] = tn(hid[:, mine], dyg[:, at]).astype(BF16)
            return carry

        lax.fori_loop(0, d // tn_cols, cols, 0)
        save_w(i, slot).start()
        return carry

    lax.fori_loop(0, ff // tm, down, 0)
    for slot in range(2):
        save_w(0, slot).wait()
    keep_x.wait()
    arrived(xg, r_x, 2)
    arrived(xg, r_x, 3)
    for k in block_sends(dy0, dyg, s_dy, r_dy) + forwards(dyg, s_dy, r_dy):
        k.wait_send()
    for k in block_sends(xst, xg, s_x, r_x) + forwards(xg, s_x, r_x):
        k.wait_send()


def weight_grad_kernel(x_ref, g_ref, o_ref):
    o_ref[...] = tn(x_ref[...], g_ref[...]).astype(BF16)


def weight_grad(x, g, tm, name):
    tokens, d = x.shape
    ff = g.shape[1]
    return pl.pallas_call(
        weight_grad_kernel, grid=(d // tm,),
        out_shape=jax.ShapeDtypeStruct((d, ff), BF16),
        in_specs=[pl.BlockSpec((tokens, tm), lambda i: (0, i)),
                  pl.BlockSpec((tokens, ff), lambda i: (0, 0), pipeline_mode=pl.Buffered(1))],
        out_specs=pl.BlockSpec((tm, ff), lambda i: (i, 0)),
        compiler_params=pltpu.CompilerParams(vmem_limit_bytes=VMEM_LIMIT),
        cost_estimate=pl.CostEstimate(flops=2 * tokens * d * ff, transcendentals=0,
                                      bytes_accessed=2 * (tokens * (d + ff) + d * ff)),
        name=name)(x, g)


def solution(mesh):
    n = mesh.shape["tp"]
    to_right = [(i, (i + 1) % n) for i in range(n)]
    to_left = [(i, (i + n - 1) % n) for i in range(n)]

    def step(x, dy, gate, up, w_gate, w_up, w_down):
        rows, d = x.shape
        tokens, ff = gate.shape
        half = rows // 2
        a_tiles, tb, tm, tn_cols = splits(ff, 1024), 512, 640, 2048
        hbm = pl.BlockSpec(memory_space=pl.ANY)

        def out(*shape, dtype=BF16):
            return jax.ShapeDtypeStruct(shape, dtype)

        ta = max(w for _, w in a_tiles)
        dma = pltpu.SemaphoreType.DMA
        xg, dg, du, own, mid, raw_l, raw_r, far_0, far_1, dwd = pl.pallas_call(
            functools.partial(gather_kernel, n, a_tiles, tb, tm, tn_cols),
            out_shape=(out(tokens, d), out(tokens, ff), out(tokens, ff), out(rows, d, dtype=F32), out(rows, d, dtype=F32),
                       out(half, d), out(half, d), out(half, d), out(half, d), out(ff, d)),
            in_specs=[hbm] * 7, out_specs=(hbm,) * 10,
            scratch_shapes=[
                pltpu.VMEM((tokens, d), BF16), pltpu.VMEM((tokens, ff), BF16),
                pltpu.VMEM((rows, ff), BF16), pltpu.VMEM((rows, ff), BF16),
                pltpu.VMEM((rows, ff), BF16), pltpu.VMEM((rows, ff), BF16),
                pltpu.VMEM((rows, d), BF16),
                pltpu.VMEM((2, ta, d), BF16), pltpu.VMEM((2, 2, tb, ff), BF16),
                pltpu.VMEM((2, rows, tb), F32), pltpu.VMEM((2, rows, tb), BF16),
                dma((4, 2)), dma((4, 2)), dma((4, 2)), dma((4, 2)),
                dma((3,)), dma((2, 2)), dma((2,)), dma((2, 2)), dma((2, 2)), dma((2,)), dma((2,)),
            ],
            compiler_params=pltpu.CompilerParams(collective_id=0, has_side_effects=True, vmem_limit_bytes=VMEM_LIMIT),
            cost_estimate=pl.CostEstimate(flops=8 * tokens * d * ff, transcendentals=tokens * ff,
                                          bytes_accessed=24 * d * ff),
            name="gather_and_rows")(dy, x, gate, up, w_down, w_gate, w_up)

        right = functools.partial(lax.ppermute, axis_name="tp", perm=to_right)
        left = functools.partial(lax.ppermute, axis_name="tp", perm=to_left)
        from_l, from_r = right(far_0), left(far_1)
        raw_from_l, raw_from_r = right(raw_r), left(raw_l)
        dw_gate = weight_grad(xg, dg, 512, "dw_gate")
        from_l, from_r, dw_gate = lax.optimization_barrier((from_l, from_r, dw_gate))
        sum_r = (mid[half:] + from_l.astype(F32)).astype(BF16)
        sum_l = (mid[:half] + from_r.astype(F32)).astype(BF16)
        sum_r, sum_l, du = lax.optimization_barrier((sum_r, sum_l, du))
        sum_from_l, sum_from_r = right(sum_r), left(sum_l)
        dw_up = weight_grad(xg, du, 512, "dw_up")
        dx = own + jnp.concatenate([sum_from_l, raw_from_l]).astype(F32) + jnp.concatenate([raw_from_r, sum_from_r]).astype(F32)
        return dx.astype(BF16), dw_gate, dw_up, dwd

    rows, cols = P(("dp", "tp"), None), P("dp", "tp")
    return jax.shard_map(
        step, mesh=mesh,
        in_specs=(rows, rows, cols, cols, P(None, "tp"), P(None, "tp"), P("tp", None)),
        out_specs=(rows, cols, cols, rows), check_vma=False)
```

```python
import functools

import jax
import jax.numpy as jnp
from jax import lax
from jax.experimental import pallas as pl
from jax.experimental.pallas import tpu as pltpu
from jax.sharding import PartitionSpec as P


BF16, F32 = jnp.bfloat16, jnp.float32
MIB = 2**20


def nt(a, b):
    return lax.dot_general(a, b, (((1,), (1,)), ((), ())), preferred_element_type=F32)


def tn(a, b):
    return lax.dot_general(a, b, (((0,), (0,)), ((), ())), preferred_element_type=F32)


def splits(total, step):
    starts = [i * step for i in range(max(total // step, 1))]
    return [(s, e - s) for s, e in zip(starts, starts[1:] + [total])]


def rows_kernel(n, a_tiles, tb, early, dy0, x0, gate, up, w_down, w_gate, w_up,
                x_left, x_right, x_next, dyg, hid, dgu, own, mid, raw_l, raw_r, far_0, far_1,
                dyv, hv, dd, gb, wa, wb, st_f, st_b,
                s_dy, r_dy, s_x, r_x, m_in, m_gu, m_wa, m_wb, m_sf, m_sb, m_d, m_h, m_dy):
    rows, d = dy0.shape
    ff = gate.shape[1]
    half = rows // 2
    me = lax.axis_index("tp")
    right, left = lax.rem(me + 1, n), lax.rem(me + n - 1, n)
    n_a, n_b = len(a_tiles), d // tb
    chunks = 4

    def rows_of(c):
        return pl.ds(pl.multiple_of(c * rows, rows), rows)

    def place(c, p):
        return pl.ds(pl.multiple_of(c * rows + p * half, half), half)

    def tile_of(j):
        return pl.ds(pl.multiple_of(j * tb, tb), tb)

    def send(src, dst, s_sem, r_sem, c, p, to):
        return pltpu.make_async_remote_copy(src_ref=src, dst_ref=dst, send_sem=s_sem.at[c, p], recv_sem=r_sem.at[c, p],
                                            device_id={"tp": to}, device_id_type=pl.DeviceIdType.MESH)

    def block_sends(src, dsts, s_sem, r_sem):
        h0, h1 = src.at[pl.ds(0, half)], src.at[pl.ds(half, half)]
        return [send(h, dst, s_sem, r_sem, c, p, to) for (h, c, p, to), dst in
                zip(((h0, 1, 0, right), (h1, 1, 1, left), (h1, 2, 0, right), (h0, 2, 1, left)), dsts)]

    def dy_sends():
        return block_sends(dy0, [dyv.at[place(c, p)] for c in (1, 2) for p in (0, 1)], s_dy, r_dy)

    def x_sends():
        return block_sends(x0, [x_left, x_right, x_next.at[pl.ds(0, half)], x_next.at[pl.ds(half, half)]], s_x, r_x)

    def forwards():
        return [send(dyv.at[place(1, p)], dyv.at[place(3, p)], s_dy, r_dy, 3, p, to) for p, to in enumerate((right, left))]

    def load_a(t):
        start, size = a_tiles[t]
        return pltpu.make_async_copy(w_down.at[pl.ds(start, size)], wa.at[pl.ds(start, size)], m_wa.at[t])

    def load_b(j, slot):
        return [pltpu.make_async_copy(w.at[tile_of(j)], wb.at[slot, :, pl.ds(k * ff, ff)], m_wb.at[slot, k])
                for k, w in enumerate((w_gate, w_up))]

    def load_gu(c, t):
        later, last = (c + 2) // 3, c // 3
        flip = (c // 2) * (1 - last)
        first, size = a_tiles[t]
        copies = []
        for p, (shift, h) in enumerate(((later * (n - 1) - last * (n - 3), flip), (later + last, 1 - flip))):
            at = pl.ds(pl.multiple_of(lax.rem(me + shift, n) * rows + h * half, half), half)
            for k, src in enumerate((gate, up)):
                copies.append(pltpu.make_async_copy(src.at[at, pl.ds(first, size)],
                                                    gb.at[t % 2, k, pl.ds(p * half, half), pl.ds(0, size)], m_gu.at[t % 2, p, k]))
        return copies

    def save_d(c):
        k = lax.rem(c, 2)
        return pltpu.make_async_copy(dd.at[rows_of(k)], dgu.at[rows_of(c)], m_d.at[k])

    def save_h(c):
        return pltpu.make_async_copy(hv, hid.at[rows_of(c)], m_h.at[0])

    def save_dy(c):
        return pltpu.make_async_copy(dyv.at[rows_of(c)], dyg.at[rows_of(c)], m_dy.at[c])

    def save_f(dst, j):
        slot = lax.rem(j, 2)
        return pltpu.make_async_copy(st_f.at[slot], dst.at[:, tile_of(j)], m_sf.at[slot])

    def save_b(dst0, dst1, j):
        slot = lax.rem(j, 2)
        return [pltpu.make_async_copy(st_b.at[slot, pl.ds(p * half, half)], dst.at[:, tile_of(j)], m_sb.at[slot, p])
                for p, dst in enumerate((dst0, dst1))]

    def start(copies):
        for k in copies:
            k.start()

    def wait(copies):
        for k in copies:
            k.wait()

    first_dy = pltpu.make_async_copy(dy0, dyv.at[pl.ds(0, rows)], m_in.at[0])
    first_dy.start()
    load_a(0).start()
    start(load_gu(0, 0))
    load_a(1).start()
    start(load_gu(0, 1))
    for t in range(2, n_a):
        load_a(t).start()

    barrier = pltpu.get_barrier_semaphore()
    for other in (left, right):
        pl.semaphore_signal(barrier, inc=1, device_id={"tp": other}, device_id_type=pl.DeviceIdType.MESH)
    pl.semaphore_wait(barrier, 2)
    start(dy_sends())
    first_dy.wait()

    def put_f(s, j, r):
        @pl.when(s * n_b + j >= 2)
        def _():
            save_f(own, j).wait()

        st_f[lax.rem(j, 2)] = r

        @pl.when(s == 0)
        def _():
            save_f(own, j).start()

        @pl.when(s == 1)
        def _():
            save_f(mid, j).start()

    def put_b(s, j, r):
        @pl.when(s * n_b + j >= 2)
        def _():
            wait(save_b(raw_l, raw_r, j))

        st_b[lax.rem(j, 2)] = r.astype(BF16)

        @pl.when(s == 0)
        def _():
            start(save_b(raw_l, raw_r, j))

        @pl.when(s == 1)
        def _():
            start(save_b(far_0, far_1, j))

    def chunk(c, carry):
        s, k = c // 2, lax.rem(c, 2)

        @pl.when(c > 0)
        def _():
            for p in range(2):
                pltpu.make_async_copy(dyv.at[place(c, p)], dyv.at[place(c, p)], r_dy.at[c, p]).wait()

        @pl.when(c == 1)
        def _():
            start(forwards())
            start(x_sends())

        @pl.when(c >= 2)
        def _():
            save_d(c).wait()

        @pl.when(c >= 1)
        def _():
            save_h(c).wait()

        save_dy(c).start()

        dy = dyv.at[rows_of(c)]
        mine = rows_of(k)
        for t, (first, size) in enumerate(a_tiles):
            @pl.when(c == 0)
            def _():
                load_a(t).wait()

            wait(load_gu(c, t))
            cols = pl.ds(first, size)
            d_hidden = nt(dy[...], wa[cols])
            g, u = (gb[t % 2, m, :, pl.ds(0, size)].astype(F32) for m in range(2))
            sig = jax.nn.sigmoid(g)
            silu = g * sig
            hv[:, cols] = (silu * u).astype(BF16)
            dd[mine, pl.ds(ff + first, size)] = (d_hidden * silu).astype(BF16)
            dd[mine, cols] = (d_hidden * u * (sig + silu * (1.0 - sig))).astype(BF16)
            if t + 2 < n_a:
                start(load_gu(c, t + 2))
            else:
                @pl.when(c < chunks - 1)
                def _():
                    start(load_gu(c + 1, t + 2 - n_a))
            if t == 1:
                @pl.when(c == 0)
                def _():
                    start(load_b(0, 0) + load_b(1, 1))

        save_d(c).start()
        save_h(c).start()

        def next_b(i):
            i2 = i + 2
            wrap = i2 // (early + n_b)

            @pl.when(s + wrap < 2)
            def _():
                i3 = i2 - wrap * (early + n_b)
                late = jnp.minimum(i3 // (2 * early), 1)
                start(load_b(lax.rem(i3, early) * (1 - late) + (i3 - early) * late, lax.rem(i, 2)))

        def one(j, carry):
            i = k * early + j
            slot = lax.rem(i, 2)
            wait(load_b(j, slot))
            r = nt(dd[mine, :], wb[slot])

            @pl.when(k == 0)
            def _():
                put_f(s, j, r)

            @pl.when(k == 1)
            def _():
                put_b(s, j, r)

            next_b(i)
            return carry

        lax.fori_loop(0, early, one, 0)

        def both(j, carry):
            i = early + j
            slot = lax.rem(i, 2)
            wait(load_b(j, slot))
            r = nt(dd[...], wb[slot])
            put_f(s, j, r[:rows])
            put_b(s, j, r[rows:])
            next_b(i)
            return carry

        lax.fori_loop(early, early + k * (n_b - early), both, 0)
        return carry

    lax.fori_loop(0, chunks, chunk, 0)

    for j in range(2):
        save_f(own, j).wait()
        wait(save_b(raw_l, raw_r, j))
        save_d(j).wait()
    save_h(0).wait()
    for c in range(chunks):
        save_dy(c).wait()
    for k in dy_sends() + forwards() + x_sends():
        k.wait_send()
    for k in x_sends():
        k.wait_recv()


def down_kernel(h_ref, dy_ref, o_ref):
    o_ref[...] = tn(h_ref[...], dy_ref[...]).astype(BF16)


def down_grad(hid, dyg, tm):
    tokens, ff = hid.shape
    d = dyg.shape[1]
    return pl.pallas_call(
        down_kernel, grid=(ff // tm,),
        out_shape=jax.ShapeDtypeStruct((ff, d), BF16),
        in_specs=[pl.BlockSpec((tokens, tm), lambda i: (0, i)),
                  pl.BlockSpec((tokens, d), lambda i: (0, 0), pipeline_mode=pl.Buffered(1))],
        out_specs=pl.BlockSpec((tm, d), lambda i: (i, 0)),
        compiler_params=pltpu.CompilerParams(vmem_limit_bytes=DOWN_MIB * MIB),
        cost_estimate=pl.CostEstimate(flops=2 * tokens * d * ff, transcendentals=0,
                                      bytes_accessed=2 * (tokens * (d + ff) + d * ff)),
        name="dw_down")(hid, dyg)


def gate_up_kernel(ff, n_x, *refs):
    x = jnp.concatenate([r[...] for r in refs[:n_x]], axis=0)
    o_gate, o_up = refs[-2:]
    r = tn(x, refs[n_x][...])
    o_gate[...] = r[:, :ff].astype(BF16)
    o_up[...] = r[:, ff:].astype(BF16)


def gate_up_grad(xs, dgu, tm, first, steps, earlier):
    tokens, ff2 = dgu.shape
    d, ff = xs[0].shape[1], ff2 // 2
    out = jax.ShapeDtypeStruct((d, ff), BF16)
    spec = pl.BlockSpec((tm, ff), lambda i: (i + first, 0))
    n_x = len(xs)
    return pl.pallas_call(
        functools.partial(gate_up_kernel, ff, n_x), grid=(steps,), out_shape=(out, out),
        in_specs=[pl.BlockSpec((x.shape[0], tm), lambda i: (0, i + first)) for x in xs]
        + [pl.BlockSpec((tokens, ff2), lambda i: (0, 0), pipeline_mode=pl.Buffered(1))]
        + [pl.BlockSpec(memory_space=pl.ANY)] * len(earlier),
        out_specs=(spec, spec),
        input_output_aliases={n_x + 1 + k: k for k in range(len(earlier))},
        compiler_params=pltpu.CompilerParams(vmem_limit_bytes=GU_MIB * MIB),
        cost_estimate=pl.CostEstimate(flops=2 * tokens * tm * steps * ff2, transcendentals=0,
                                      bytes_accessed=2 * (tokens * (tm * steps + ff2) + tm * steps * ff2)),
        name="dw_gate_up")(*xs, dgu, *earlier)


DOWN_MIB, GU_MIB = 40, 34


def solution(mesh):
    n = mesh.shape["tp"]
    to_right = [(i, (i + 1) % n) for i in range(n)]
    to_left = [(i, (i + n - 1) % n) for i in range(n)]

    def step(x, dy, gate, up, w_gate, w_up, w_down):
        rows, d = x.shape
        tokens, ff = gate.shape
        half = rows // 2
        a_tiles, tb, early, tm, td = splits(ff, 768), 512, 2, 256, 640
        hbm = pl.BlockSpec(memory_space=pl.ANY)

        def out(*shape, dtype=BF16):
            return jax.ShapeDtypeStruct(shape, dtype)

        ta = max(w for _, w in a_tiles)
        assert len(a_tiles) % 2 == 0 and early % 2 == 0
        dma, vmem = pltpu.SemaphoreType.DMA, pltpu.VMEM
        x_left, x_right, x_next, dyg, hid, dgu, own, mid, raw_l, raw_r, far_0, far_1 = pl.pallas_call(
            functools.partial(rows_kernel, n, a_tiles, tb, early),
            out_shape=(out(half, d), out(half, d), out(rows, d), out(tokens, d), out(tokens, ff), out(tokens, 2 * ff),
                       out(rows, d, dtype=F32), out(rows, d, dtype=F32),
                       out(half, d), out(half, d), out(half, d), out(half, d)),
            in_specs=[hbm] * 7, out_specs=(hbm,) * 12,
            scratch_shapes=[
                vmem((tokens, d), BF16), vmem((rows, ff), BF16), vmem((2 * rows, 2 * ff), BF16),
                vmem((2, 2, rows, ta), BF16), vmem((ff, d), BF16), vmem((2, tb, 2 * ff), BF16),
                vmem((2, rows, tb), F32), vmem((2, rows, tb), BF16),
                dma((4, 2)), dma((4, 2)), dma((3, 2)), dma((3, 2)),
                dma((1,)), dma((2, 2, 2)), dma((len(a_tiles),)), dma((2, 2)), dma((2,)), dma((2, 2)), dma((2,)), dma((1,)), dma((4,)),
            ],
            compiler_params=pltpu.CompilerParams(collective_id=0, has_side_effects=True, vmem_limit_bytes=67_000_000),
            cost_estimate=pl.CostEstimate(flops=6 * tokens * d * ff, transcendentals=tokens * ff,
                                          bytes_accessed=16 * d * ff),
            name="rows")(dy, x, gate, up, w_down, w_gate, w_up)

        def hop(array, to):
            return lax.ppermute(array, "tp", to)

        x_far_0, x_far_1 = hop(x_left, to_right), hop(x_right, to_left)
        from_l, from_r = hop(far_0, to_right), hop(far_1, to_left)
        raw_from_l, raw_from_r = hop(raw_r, to_right), hop(raw_l, to_left)
        dw_down = down_grad(hid, dyg, td)
        x_far_0, x_far_1, dw_down = lax.optimization_barrier((x_far_0, x_far_1, dw_down))
        xs = (x, x_left, x_right, x_next, x_far_0, x_far_1)
        steps = d // tm
        cut = steps // 2
        dw = gate_up_grad(xs, dgu, tm, 0, cut, ())
        from_l, from_r, dw = lax.optimization_barrier((from_l, from_r, dw))
        sum_r = (mid[half:] + from_l.astype(F32)).astype(BF16)
        sum_l = (mid[:half] + from_r.astype(F32)).astype(BF16)
        sum_r, sum_l, dw = lax.optimization_barrier((sum_r, sum_l, dw))
        sum_from_l, sum_from_r = hop(sum_r, to_right), hop(sum_l, to_left)
        dw_gate, dw_up = gate_up_grad(xs, dgu, tm, cut, steps - cut, dw)
        dx = own + jnp.concatenate([sum_from_l, raw_from_l]).astype(F32) + jnp.concatenate([raw_from_r, sum_from_r]).astype(F32)
        return dx.astype(BF16), dw_gate, dw_up, dw_down

    rows, cols = P(("dp", "tp"), None), P("dp", "tp")
    return jax.shard_map(
        step, mesh=mesh,
        in_specs=(rows, rows, cols, cols, P(None, "tp"), P(None, "tp"), P("tp", None)),
        out_specs=(rows, cols, cols, rows), check_vma=False)
```

```python
import functools

import jax
import jax.numpy as jnp
from jax import lax
from jax.experimental import pallas as pl
from jax.experimental.pallas import tpu as pltpu
from jax.sharding import PartitionSpec as P


BF16, F32 = jnp.bfloat16, jnp.float32
MIB = 2**20


def nt(a, b):
    return lax.dot_general(a, b, (((1,), (1,)), ((), ())), preferred_element_type=F32)


def tn(a, b):
    return lax.dot_general(a, b, (((0,), (0,)), ((), ())), preferred_element_type=F32)


def splits(total, step):
    starts = [i * step for i in range(max(total // step, 1))]
    return [(s, e - s) for s, e in zip(starts, starts[1:] + [total])]


def rows_kernel(n, a_tiles, tb, early, dy0, x0, gate, up, w_down, w_gate, w_up,
                x_left, x_right, x_next, dyg, hid, dgu, own, mid, out_r, out_l,
                dyv, hv, dd, gb, wa, wb, st_f, st_b,
                s_dy, r_dy, s_x, r_x, m_in, m_gu, m_wa, m_wb, m_sf, m_sb, m_d, m_h, m_dy):
    rows, d = dy0.shape
    ff = gate.shape[1]
    half = rows // 2
    me = lax.axis_index("tp")
    right, left = lax.rem(me + 1, n), lax.rem(me + n - 1, n)
    n_a, n_b = len(a_tiles), d // tb
    chunks = 4

    def rows_of(c):
        return pl.ds(pl.multiple_of(c * rows, rows), rows)

    def place(c, p):
        return pl.ds(pl.multiple_of(c * rows + p * half, half), half)

    def tile_of(j):
        return pl.ds(pl.multiple_of(j * tb, tb), tb)

    def send(src, dst, s_sem, r_sem, c, p, to):
        return pltpu.make_async_remote_copy(src_ref=src, dst_ref=dst, send_sem=s_sem.at[c, p], recv_sem=r_sem.at[c, p],
                                            device_id={"tp": to}, device_id_type=pl.DeviceIdType.MESH)

    def block_sends(src, dsts, s_sem, r_sem):
        h0, h1 = src.at[pl.ds(0, half)], src.at[pl.ds(half, half)]
        return [send(h, dst, s_sem, r_sem, c, p, to) for (h, c, p, to), dst in
                zip(((h0, 1, 0, right), (h1, 1, 1, left), (h1, 2, 0, right), (h0, 2, 1, left)), dsts)]

    def dy_sends():
        return block_sends(dy0, [dyv.at[place(c, p)] for c in (1, 2) for p in (0, 1)], s_dy, r_dy)

    def x_sends():
        return block_sends(x0, [x_left, x_right, x_next.at[pl.ds(0, half)], x_next.at[pl.ds(half, half)]], s_x, r_x)

    def forwards():
        return [send(dyv.at[place(1, p)], dyv.at[place(3, p)], s_dy, r_dy, 3, p, to) for p, to in enumerate((right, left))]

    def load_a(t):
        start, size = a_tiles[t]
        return pltpu.make_async_copy(w_down.at[pl.ds(start, size)], wa.at[pl.ds(start, size)], m_wa.at[t])

    def load_b(j, slot):
        return [pltpu.make_async_copy(w.at[tile_of(j)], wb.at[slot, :, pl.ds(k * ff, ff)], m_wb.at[slot, k])
                for k, w in enumerate((w_gate, w_up))]

    def load_gu(c, t):
        later, last = (c + 2) // 3, c // 3
        flip = (c // 2) * (1 - last)
        first, size = a_tiles[t]
        copies = []
        for p, (shift, h) in enumerate(((later * (n - 1) - last * (n - 3), flip), (later + last, 1 - flip))):
            at = pl.ds(pl.multiple_of(lax.rem(me + shift, n) * rows + h * half, half), half)
            for k, src in enumerate((gate, up)):
                copies.append(pltpu.make_async_copy(src.at[at, pl.ds(first, size)],
                                                    gb.at[t % 2, k, pl.ds(p * half, half), pl.ds(0, size)], m_gu.at[t % 2, p, k]))
        return copies

    def save_d(c):
        k = lax.rem(c, 2)
        return pltpu.make_async_copy(dd.at[rows_of(k)], dgu.at[rows_of(c)], m_d.at[k])

    def save_h(c):
        return pltpu.make_async_copy(hv, hid.at[rows_of(c)], m_h.at[0])

    def save_dy(c):
        return pltpu.make_async_copy(dyv.at[rows_of(c)], dyg.at[rows_of(c)], m_dy.at[c])

    def save_f(dst, j):
        slot = lax.rem(j, 2)
        return pltpu.make_async_copy(st_f.at[slot], dst.at[:, tile_of(j)], m_sf.at[slot])

    def save_b(near, j):
        slot = lax.rem(j, 2)
        dsts = (out_l, out_r) if near else (out_r, out_l)
        return [pltpu.make_async_copy(st_b.at[slot, pl.ds(p * half, half)],
                                      dst.at[pl.ds(half if near else 0, half), tile_of(j)], m_sb.at[slot, p])
                for p, dst in enumerate(dsts)]

    def start(copies):
        for k in copies:
            k.start()

    def wait(copies):
        for k in copies:
            k.wait()

    first_dy = pltpu.make_async_copy(dy0, dyv.at[pl.ds(0, rows)], m_in.at[0])
    first_dy.start()
    load_a(0).start()
    start(load_gu(0, 0))
    load_a(1).start()
    start(load_gu(0, 1))
    for t in range(2, n_a):
        load_a(t).start()

    barrier = pltpu.get_barrier_semaphore()
    for other in (left, right):
        pl.semaphore_signal(barrier, inc=1, device_id={"tp": other}, device_id_type=pl.DeviceIdType.MESH)
    pl.semaphore_wait(barrier, 2)
    start(dy_sends())
    first_dy.wait()

    def put_f(s, j, r):
        @pl.when(s * n_b + j >= 2)
        def _():
            save_f(own, j).wait()

        st_f[lax.rem(j, 2)] = r

        @pl.when(s == 0)
        def _():
            save_f(own, j).start()

        @pl.when(s == 1)
        def _():
            save_f(mid, j).start()

    def put_b(s, j, r):
        @pl.when(s * n_b + j >= 2)
        def _():
            wait(save_b(True, j))

        st_b[lax.rem(j, 2)] = r.astype(BF16)

        @pl.when(s == 0)
        def _():
            start(save_b(True, j))

        @pl.when(s == 1)
        def _():
            start(save_b(False, j))

    def chunk(c, carry):
        s, k = c // 2, lax.rem(c, 2)

        @pl.when(c > 0)
        def _():
            for p in range(2):
                pltpu.make_async_copy(dyv.at[place(c, p)], dyv.at[place(c, p)], r_dy.at[c, p]).wait()

        @pl.when(c == 1)
        def _():
            start(forwards())
            start(x_sends())

        @pl.when(c >= 2)
        def _():
            save_d(c).wait()

        @pl.when(c >= 1)
        def _():
            save_h(c).wait()

        save_dy(c).start()

        dy = dyv.at[rows_of(c)]
        mine = rows_of(k)
        for t, (first, size) in enumerate(a_tiles):
            @pl.when(c == 0)
            def _():
                load_a(t).wait()

            wait(load_gu(c, t))
            cols = pl.ds(first, size)
            d_hidden = nt(dy[...], wa[cols])
            g, u = (gb[t % 2, m, :, pl.ds(0, size)].astype(F32) for m in range(2))
            sig = jax.nn.sigmoid(g)
            silu = g * sig
            hv[:, cols] = (silu * u).astype(BF16)
            dd[mine, pl.ds(ff + first, size)] = (d_hidden * silu).astype(BF16)
            dd[mine, cols] = (d_hidden * u * (sig + silu * (1.0 - sig))).astype(BF16)
            if t + 2 < n_a:
                start(load_gu(c, t + 2))
            else:
                @pl.when(c < chunks - 1)
                def _():
                    start(load_gu(c + 1, t + 2 - n_a))
            if t == 1:
                @pl.when(c == 0)
                def _():
                    start(load_b(0, 0) + load_b(1, 1))

        save_d(c).start()
        save_h(c).start()

        def next_b(i):
            i2 = i + 2
            wrap = i2 // (early + n_b)

            @pl.when(s + wrap < 2)
            def _():
                i3 = i2 - wrap * (early + n_b)
                late = jnp.minimum(i3 // (2 * early), 1)
                start(load_b(lax.rem(i3, early) * (1 - late) + (i3 - early) * late, lax.rem(i, 2)))

        def one(j, carry):
            i = k * early + j
            slot = lax.rem(i, 2)
            wait(load_b(j, slot))
            r = nt(dd[mine, :], wb[slot])

            @pl.when(k == 0)
            def _():
                put_f(s, j, r)

            @pl.when(k == 1)
            def _():
                put_b(s, j, r)

            next_b(i)
            return carry

        lax.fori_loop(0, early, one, 0)

        def both(j, carry):
            i = early + j
            slot = lax.rem(i, 2)
            wait(load_b(j, slot))
            r = nt(dd[...], wb[slot])
            put_f(s, j, r[:rows])
            put_b(s, j, r[rows:])
            next_b(i)
            return carry

        lax.fori_loop(early, early + k * (n_b - early), both, 0)
        return carry

    lax.fori_loop(0, chunks, chunk, 0)

    for j in range(2):
        save_f(own, j).wait()
        wait(save_b(True, j))
        save_d(j).wait()
    save_h(0).wait()
    for c in range(chunks):
        save_dy(c).wait()
    for k in dy_sends() + forwards() + x_sends():
        k.wait_send()
    for k in x_sends():
        k.wait_recv()


def down_kernel(h_ref, dy_ref, o_ref):
    o_ref[...] = tn(h_ref[...], dy_ref[...]).astype(BF16)


def down_grad(hid, dyg, tm):
    tokens, ff = hid.shape
    d = dyg.shape[1]
    return pl.pallas_call(
        down_kernel, grid=(ff // tm,),
        out_shape=jax.ShapeDtypeStruct((ff, d), BF16),
        in_specs=[pl.BlockSpec((tokens, tm), lambda i: (0, i)),
                  pl.BlockSpec((tokens, d), lambda i: (0, 0), pipeline_mode=pl.Buffered(1))],
        out_specs=pl.BlockSpec((tm, d), lambda i: (i, 0)),
        compiler_params=pltpu.CompilerParams(vmem_limit_bytes=DOWN_MIB * MIB),
        cost_estimate=pl.CostEstimate(flops=2 * tokens * d * ff, transcendentals=0,
                                      bytes_accessed=2 * (tokens * (d + ff) + d * ff)),
        name="dw_down")(hid, dyg)


def gate_up_kernel(ff, n_x, *refs):
    x = jnp.concatenate([r[...] for r in refs[:n_x]], axis=0)
    o_gate, o_up = refs[-2:]
    r = tn(x, refs[n_x][...])
    o_gate[...] = r[:, :ff].astype(BF16)
    o_up[...] = r[:, ff:].astype(BF16)


def gate_up_grad(xs, dgu, tm, first, steps, earlier):
    tokens, ff2 = dgu.shape
    d, ff = xs[0].shape[1], ff2 // 2
    out = jax.ShapeDtypeStruct((d, ff), BF16)
    spec = pl.BlockSpec((tm, ff), lambda i: (i + first, 0))
    n_x = len(xs)
    return pl.pallas_call(
        functools.partial(gate_up_kernel, ff, n_x), grid=(steps,), out_shape=(out, out),
        in_specs=[pl.BlockSpec((x.shape[0], tm), lambda i: (0, i + first)) for x in xs]
        + [pl.BlockSpec((tokens, ff2), lambda i: (0, 0), pipeline_mode=pl.Buffered(1))]
        + [pl.BlockSpec(memory_space=pl.ANY)] * len(earlier),
        out_specs=(spec, spec),
        input_output_aliases={n_x + 1 + k: k for k in range(len(earlier))},
        compiler_params=pltpu.CompilerParams(vmem_limit_bytes=GU_MIB * MIB),
        cost_estimate=pl.CostEstimate(flops=2 * tokens * tm * steps * ff2, transcendentals=0,
                                      bytes_accessed=2 * (tokens * (tm * steps + ff2) + tm * steps * ff2)),
        name="dw_gate_up")(*xs, dgu, *earlier)


DOWN_MIB, GU_MIB = 28, 24


def solution(mesh):
    n = mesh.shape["tp"]
    to_right = [(i, (i + 1) % n) for i in range(n)]
    to_left = [(i, (i + n - 1) % n) for i in range(n)]

    def step(x, dy, gate, up, w_gate, w_up, w_down):
        rows, d = x.shape
        tokens, ff = gate.shape
        half = rows // 2
        a_tiles, tb, early, tm, td = splits(ff, 768), 512, 2, 256, 640
        hbm = pl.BlockSpec(memory_space=pl.ANY)

        def out(*shape, dtype=BF16):
            return jax.ShapeDtypeStruct(shape, dtype)

        ta = max(w for _, w in a_tiles)
        assert len(a_tiles) % 2 == 0 and early % 2 == 0
        dma, vmem = pltpu.SemaphoreType.DMA, pltpu.VMEM
        x_left, x_right, x_next, dyg, hid, dgu, own, mid, out_r, out_l = pl.pallas_call(
            functools.partial(rows_kernel, n, a_tiles, tb, early),
            out_shape=(out(half, d), out(half, d), out(rows, d), out(tokens, d), out(tokens, ff), out(tokens, 2 * ff),
                       out(rows, d, dtype=F32), out(rows, d, dtype=F32),
                       out(rows, d), out(rows, d)),
            in_specs=[hbm] * 7, out_specs=(hbm,) * 10,
            scratch_shapes=[
                vmem((tokens, d), BF16), vmem((rows, ff), BF16), vmem((2 * rows, 2 * ff), BF16),
                vmem((2, 2, rows, ta), BF16), vmem((ff, d), BF16), vmem((2, tb, 2 * ff), BF16),
                vmem((2, rows, tb), F32), vmem((2, rows, tb), BF16),
                dma((4, 2)), dma((4, 2)), dma((3, 2)), dma((3, 2)),
                dma((1,)), dma((2, 2, 2)), dma((len(a_tiles),)), dma((2, 2)), dma((2,)), dma((2, 2)), dma((2,)), dma((1,)), dma((4,)),
            ],
            compiler_params=pltpu.CompilerParams(collective_id=0, has_side_effects=True, vmem_limit_bytes=67_000_000),
            cost_estimate=pl.CostEstimate(flops=6 * tokens * d * ff, transcendentals=tokens * ff,
                                          bytes_accessed=16 * d * ff),
            name="rows")(dy, x, gate, up, w_down, w_gate, w_up)

        def hop(array, to):
            return lax.ppermute(array, "tp", to)

        x_far_0, x_far_1 = hop(x_left, to_right), hop(x_right, to_left)
        from_l, from_r = hop(out_r, to_right), hop(out_l, to_left)
        dw_down = down_grad(hid, dyg, td)
        x_far_0, x_far_1, dw_down = lax.optimization_barrier((x_far_0, x_far_1, dw_down))
        xs = (x, x_left, x_right, x_next, x_far_0, x_far_1)
        steps = d // tm
        cut = steps // 2
        dw = gate_up_grad(xs, dgu, tm, 0, cut, ())
        from_l, from_r, dw = lax.optimization_barrier((from_l, from_r, dw))
        sum_r = (mid[half:] + from_l[:half].astype(F32)).astype(BF16)
        sum_l = (mid[:half] + from_r[:half].astype(F32)).astype(BF16)
        sum_r, sum_l, dw = lax.optimization_barrier((sum_r, sum_l, dw))
        sum_from_l, sum_from_r = hop(sum_r, to_right), hop(sum_l, to_left)
        dw_gate, dw_up = gate_up_grad(xs, dgu, tm, cut, steps - cut, dw)
        top = own[:half] + sum_from_l.astype(F32) + from_r[half:].astype(F32)
        bottom = own[half:] + from_l[half:].astype(F32) + sum_from_r.astype(F32)
        dx = jnp.concatenate([top.astype(BF16), bottom.astype(BF16)])
        return dx, dw_gate, dw_up, dw_down

    rows, cols = P(("dp", "tp"), None), P("dp", "tp")
    return jax.shard_map(
        step, mesh=mesh,
        in_specs=(rows, rows, cols, cols, P(None, "tp"), P(None, "tp"), P("tp", None)),
        out_specs=(rows, cols, cols, rows), check_vma=False)
```
